32 devices in a mesh: grp: 4 (over y, core), sub: 8 (over z, x).
Axes of the slice: x: 2, y: 2, z: 4, core: 2. Of those that a mesh axis runs over, the one named last changes fastest.
Arguments:
- fields: float32 [4, 35, 8192], P(None, None, ('grp', 'sub')), may hold values from -6 to 6
- section_store: float32 [4, 35, 8192], P(None, None, ('grp', 'sub')), may hold values from -6 to 6
- metric_terms: float32 [9, 8192], P(None, ('grp', 'sub')), may hold values from -6 to 6
- normals: float32 [4, 3, 8192], P(None, None, ('grp', 'sub')), may hold values from -3 to 3
- face_scale: float32 [4, 8192], P(None, ('grp', 'sub')), may hold values from 1 to 4
- damping: float32 [8192], P(('grp', 'sub')), may hold values from 1 to 10
- absorb_mask: int32 [8192], P(('grp', 'sub')), may hold values from 0 to 1
- refine_level: int32 [8192], P(('grp', 'sub')), may hold values from 0 to 2
- face_source: int32 [4, 8192], P(None, ('grp', 'sub')), may hold values from -1 to 1343, as said below
- orientation: int32 [4, 8192], P(None, ('grp', 'sub')), may hold values from 0 to 5, as said below
- derivative: float32 [3, 35, 35], replicated, may hold values from -1 to 1
- lift_matrix: float32 [35, 60], replicated, may hold values from -0.75 to 0.75
Outputs:
- fields_next: float32 [4, 35, 8192], P(None, None, ('grp', 'sub'))
- store_next: float32 [4, 35, 8192], P(None, None, ('grp', 'sub'))
- absorbed_energy: float32 [], replicated
The draws below stay inside these ranges and needn't reach their ends.
Inputs may be any that keep to these rules, and one draw needn't show every extreme that they name: `face_source`: the neighbour relation is symmetric: the neighbour of a face's neighbour is the face itself, every code at or above 1024 names a slot used by exactly one face of its device, and a face's neighbour on device d holds the matching slot as in the reference program. A device uses the slots of a block from rank 0 on without gaps; it never uses block s (its own sub index), nor block 8 at the first grp index or block 9 at the last. For a sub peer b with |b - s| <= 4 at most 32 ranks are used, for other peers at most 8, and across grp at most 32; in every draw some near pair uses all 32, some farther pair all 8, and some pair across grp all 32. Local neighbours lie on the same device. `orientation`: paired faces have inverse orientations: 1 and 2 swap, 0, 3, 4 and 5 stay.
All inputs are finite; a program needn't handle non-finite values.
Results may differ from the reference program's by a relative error of at most 0.0003.
Values sent between devices are 32-bit elements; how exact they have to be, the bound alone decides.
No kernel may reach another device: no remote copies, remote signals or barrier semaphores. Data moves between devices by JAX's collectives and lax.ppermute only.
A program may use at most 64 MiB of HBM per device.

```python
import math
import jax
import jax.numpy as jnp
import numpy as np
from jax import lax

VOLUME_NODES = 35
FACE_NODES = 15
NEAR_PEERS = 4
LOCAL_ELEMENTS = 256
PEER_SLOTS = 32
ELEMENTS = 8192
N_GRP = 4
N_SUB = 8


def link_tables(key):
    devices = N_GRP * N_SUB
    per_device = LOCAL_ELEMENTS
    slot_width = PEER_SLOTS
    narrow = slot_width // 4
    block_total = N_SUB + 2
    box_size = block_total * slot_width
    face_total = 4 * per_device
    subkeys = jax.random.split(jax.random.fold_in(key, 7301), 10)
    member_ids = jnp.arange(N_SUB, dtype=jnp.int32)
    spread = jnp.abs(member_ids[:, None] - member_ids[None, :])
    near_draw = jax.random.randint(subkeys[0], (N_GRP, N_SUB, N_SUB), slot_width // 2, slot_width + 1)
    far_draw = jax.random.randint(subkeys[1], (N_GRP, N_SUB, N_SUB), 0, narrow + 1)
    upper_part = jnp.triu(jnp.where(spread[None] <= NEAR_PEERS, near_draw, far_draw), 1)
    counts = upper_part + jnp.transpose(upper_part, (0, 2, 1))
    start_at = jax.random.randint(subkeys[2], (N_GRP,), 0, N_SUB - NEAR_PEERS - 1)
    group_ids = jnp.arange(N_GRP, dtype=jnp.int32)
    counts = counts.at[group_ids, start_at, start_at + 1].set(slot_width)
    counts = counts.at[group_ids, start_at + 1, start_at].set(slot_width)
    counts = counts.at[group_ids, start_at, start_at + NEAR_PEERS + 1].set(narrow)
    counts = counts.at[group_ids, start_at + NEAR_PEERS + 1, start_at].set(narrow)
    slab_counts = jax.random.randint(subkeys[3], (N_GRP - 1, N_SUB), slot_width // 2, slot_width + 1)
    slab_group = jax.random.randint(subkeys[4], (), 0, N_GRP - 1)
    slab_member = jax.random.randint(subkeys[5], (), 0, N_SUB)
    slab_counts = slab_counts.at[slab_group, slab_member].set(slot_width)
    zero_row = jnp.zeros((1, N_SUB), jnp.int32)
    down_counts = jnp.concatenate([zero_row, slab_counts], 0).reshape(devices)
    upward = jnp.concatenate([slab_counts, zero_row], 0).reshape(devices)
    block_counts = jnp.concatenate([counts.reshape(devices, N_SUB), down_counts[:, None], upward[:, None]], 1)
    block_ends = jnp.cumsum(block_counts, 1)
    begins = block_ends - block_counts
    remote_total = block_ends[:, -1]
    leftover = face_total - remote_total
    wall_draw = jax.random.randint(subkeys[6], (devices,), 0, 1 << 20)
    wall_count = leftover % 2 + 2 * (wall_draw % (leftover // 16 + 1))
    pair_start = remote_total + wall_count
    position = jnp.arange(face_total, dtype=jnp.int32)
    block_index = jax.vmap(lambda row: jnp.searchsorted(row, position, side='right'))(block_ends).astype(jnp.int32)
    block_index = jnp.minimum(block_index, block_total - 1)
    rank = position[None, :] - jnp.take_along_axis(begins, block_index, 1)
    is_remote = position[None, :] < remote_total[:, None]
    is_pair = position[None, :] >= pair_start[:, None]
    offset_pair = position[None, :] - pair_start[:, None]
    partner_pos = jnp.clip(pair_start[:, None] + jnp.bitwise_xor(offset_pair, 1), 0, face_total - 1)
    orders = jax.vmap(lambda sub_key: jax.random.permutation(sub_key, face_total))(jax.random.split(subkeys[7], devices)).astype(jnp.int32)
    partner_face = jnp.take_along_axis(orders, partner_pos, 1)
    code_pos = jnp.where(is_remote, face_total + block_index * slot_width + rank, jnp.where(is_pair, partner_face, -1))
    inverse = jnp.array([0, 2, 1, 3, 4, 5], jnp.int32)
    own_turn = jax.random.randint(subkeys[8], (devices, face_total), 0, 6)
    pair_lead = offset_pair % 2 == 0
    local_turn = jnp.where(pair_lead, own_turn, inverse[jnp.take_along_axis(own_turn, partner_pos, 1)])
    link_turn = jax.random.randint(subkeys[9], (devices * box_size,), 0, 6)
    device = jnp.arange(devices, dtype=jnp.int32)[:, None]
    group_index = device // N_SUB
    member = device % N_SUB
    peer_dev = jnp.where(block_index < N_SUB, group_index * N_SUB + block_index, jnp.where(block_index == N_SUB, device - N_SUB, device + N_SUB))
    peer_slot = jnp.where(block_index < N_SUB, member * slot_width + rank, jnp.where(block_index == N_SUB, (N_SUB + 1) * slot_width + rank, N_SUB * slot_width + rank))
    own_slot = block_index * slot_width + rank
    mine = link_turn[jnp.clip(device * box_size + own_slot, 0, devices * box_size - 1)]
    theirs = inverse[link_turn[jnp.clip(peer_dev * box_size + peer_slot, 0, devices * box_size - 1)]]
    remote_turn = jnp.where(device < peer_dev, mine, theirs)
    turn_pos = jnp.where(is_remote, remote_turn, jnp.where(is_pair, local_turn, own_turn))
    device_rows = jnp.broadcast_to(device, (devices, face_total))
    source_faces = jnp.zeros((devices, face_total), jnp.int32).at[device_rows, orders].set(code_pos)
    turn_faces = jnp.zeros((devices, face_total), jnp.int32).at[device_rows, orders].set(turn_pos)
    source_out = jnp.transpose(source_faces.reshape(devices, 4, per_device), (1, 0, 2)).reshape(4, devices * per_device)
    turn_out = jnp.transpose(turn_faces.reshape(devices, 4, per_device), (1, 0, 2)).reshape(4, devices * per_device)
    return (source_out, turn_out)


def draw_face_source(key, part):
    return link_tables(key)[0]


def draw_orientation(key, part):
    return link_tables(key)[1]


def draw_absorb_mask(key, part):
    total_elements = LOCAL_ELEMENTS * N_GRP * N_SUB
    element = jnp.arange(total_elements, dtype=jnp.int32)
    limit = 150 + 300 * element // total_elements
    picks = jax.random.randint(jax.random.fold_in(key, 4409), (total_elements,), 0, 1000)
    return (picks < limit).astype(jnp.int32)


def plant(result, rng, least, high):
    extent = result.shape
    place = [jax.random.randint(jax.random.fold_in(rng, axis), (), 0, extent[axis]) for axis in range(len(extent))]
    result = result.at[tuple(place)].set(least)
    longest = extent.index(max(extent))
    place[longest] = (place[longest] + 1) % extent[longest]
    return result.at[tuple(place)].set(high)


def block_scale(key, dims, shards, smallest, high):
    loudness, own = 1.0, jax.random.fold_in(key, 6)
    for axis_at, parts in shards:
        heights = jnp.exp(jax.random.uniform(jax.random.fold_in(own, axis_at), (parts,), jnp.float32, smallest / len(shards), high / len(shards)))
        loudness = loudness * jnp.repeat(heights, dims[axis_at] // parts).reshape([-1 if axis == axis_at else 1 for axis in range(len(dims))])
    return loudness


def centred(key, extent, scale, reach, shards=(), kind=jnp.bfloat16):
    values = jax.random.normal(key, extent, jnp.float32) * scale
    if len(shards) > 0:
        values = block_scale(key, extent, shards, -0.22, 0.18) * values
    return jnp.clip(values, min=-reach, max=reach).astype(kind)


def setup_inputs(seed: int = 0) -> dict:
    key_list = jax.random.split(jax.random.key(seed), 13)
    fields = centred(key_list[0], (4, VOLUME_NODES, ELEMENTS), 1.0, 6.0, ((2, 32),), jnp.float32)
    section_store = centred(key_list[1], (4, VOLUME_NODES, ELEMENTS), 1.0, 6.0, ((2, 32),), jnp.float32)
    metric_terms = centred(key_list[2], (9, ELEMENTS), 1.0, 6.0, ((1, 32),), jnp.float32)
    normals = centred(key_list[3], (4, 3, ELEMENTS), 0.577, 3.0, ((2, 32),), jnp.float32)
    face_scale = jnp.clip(jnp.exp(math.log(4.0) - 1.3862944 * jax.random.uniform(key_list[4], (4, ELEMENTS), jnp.float32) ** block_scale(key_list[4], (4, ELEMENTS), ((1, 32),), -0.2, 0.2)), 1.0, 4.0)
    damping = jnp.clip(jnp.exp(math.log(10.0) - 2.3025851 * jax.random.uniform(key_list[5], (ELEMENTS,), jnp.float32) ** block_scale(key_list[5], (ELEMENTS,), ((0, 32),), -0.2, 0.2)), 1.0, 10.0)
    absorb_mask = draw_absorb_mask(jax.random.fold_in(key_list[12], 71), 0)
    refine_level = plant(jax.random.randint(key_list[7], (ELEMENTS,), 0, 3), jax.random.fold_in(key_list[7], 1), 0, 2).astype(jnp.int32)
    face_source = draw_face_source(jax.random.fold_in(key_list[12], 71), 0)
    orientation = draw_orientation(jax.random.fold_in(key_list[12], 71), 0)
    derivative = centred(key_list[10], (3, VOLUME_NODES, VOLUME_NODES), VOLUME_NODES ** -0.5, 1.0, (), jnp.float32)
    lift_matrix = centred(key_list[11], (VOLUME_NODES, 4 * FACE_NODES), (4 * FACE_NODES) ** -0.5, 0.75, (), jnp.float32)
    return dict(fields=fields, section_store=section_store, metric_terms=metric_terms, normals=normals, face_scale=face_scale, damping=damping, absorb_mask=absorb_mask, refine_level=refine_level, face_source=face_source, orientation=orientation, derivative=derivative, lift_matrix=lift_matrix)


RUNGE_CARRY = -567301805773.0 / 1357537059087.0
RUNGE_ADVANCE = 5161836677717.0 / 13612068292357.0
TIME_STEP = 0.02


def node_tables():
    volume_list = [(first_part, second_part, third_part, 4 - first_part - second_part - third_part)
                   for first_part in range(5) for second_part in range(5 - first_part)
                   for third_part in range(5 - first_part - second_part)]
    triples = [(first_part, second_part, 4 - first_part - second_part)
               for first_part in range(5) for second_part in range(5 - first_part)]
    face_index = np.zeros((4, 15), np.int32)
    for facet in range(4):
        others = [corner for corner in range(4) if corner != facet]
        for node_pos in range(15):
            corners = [0, 0, 0, 0]
            for place_pos in range(3):
                corners[others[place_pos]] = triples[node_pos][place_pos]
            face_index[facet, node_pos] = volume_list.index(tuple(corners))
    vertex_orders = [(0, 1, 2), (1, 2, 0), (2, 0, 1), (0, 2, 1), (2, 1, 0), (1, 0, 2)]
    turn_index = np.zeros((6, 15), np.int32)
    for option in range(6):
        vertex_order = vertex_orders[option]
        for node_pos in range(15):
            triple = triples[node_pos]
            turned = (triple[vertex_order[0]], triple[vertex_order[1]], triple[vertex_order[2]])
            turn_index[option, node_pos] = triples.index(turned)
    return face_index, turn_index


def turn_matrices():
    face_index, turn_index = node_tables()
    table = np.zeros((6, 15, 15), np.float32)
    for option in range(6):
        for node_pos in range(15):
            table[option, node_pos, turn_index[option, node_pos]] = 1.0
    return jnp.asarray(table, jnp.float32)


def advance(fields, section_store, metric_terms, normals, face_scale, damping, absorb_mask, refine_level,
            face_codes, orient_flat, inner_cols, outer_cols, derivative, lift_matrix):
    elements_here = fields.shape[2]
    total_faces = 4 * elements_here
    turning = turn_matrices()
    inside = inner_cols.reshape(4, FACE_NODES, total_faces)
    gathered = outer_cols.reshape(4, FACE_NODES, total_faces)
    outside = gathered
    for option in range(1, 6):
        turned = jnp.einsum("jk,ckx->cjx", turning[option], gathered, precision=lax.Precision.HIGHEST)
        outside = jnp.where(orient_flat[None, None, :] == option, turned, outside)
    normal_flat = jnp.transpose(normals, (1, 0, 2)).reshape(3, total_faces)
    on_wall = (face_codes < 0)[None, :]
    press_in = inside[0]
    veloc_in = inside[1:]
    normal_in = jnp.sum(normal_flat[:, None, :] * veloc_in, 0)
    press_out = jnp.where(on_wall, press_in, outside[0])
    veloc_out = jnp.where(on_wall[None], veloc_in - 2.0 * normal_flat[:, None, :] * normal_in[None], outside[1:])
    press_jump = press_in - press_out
    normal_jump = jnp.sum(normal_flat[:, None, :] * (veloc_in - veloc_out), 0)
    growth = jnp.exp2(refine_level.astype(jnp.float32))
    weight_face = (face_scale * growth[None, :]).reshape(total_faces)
    flux_press = 0.5 * weight_face[None, :] * (normal_jump - press_jump)
    flux_veloc = 0.5 * weight_face[None, None, :] * normal_flat[:, None, :] * (press_jump - normal_jump)[None]
    flux_all = jnp.concatenate([flux_press[None], flux_veloc], 0).reshape(4, FACE_NODES, 4, elements_here)
    lifted = jnp.einsum("nfj,cjfe->cne", lift_matrix.reshape(VOLUME_NODES, 4, FACE_NODES), flux_all,
                        precision=lax.Precision.HIGHEST)
    slopes = jnp.einsum("dnm,cme->dcne", derivative, fields, precision=lax.Precision.HIGHEST)
    metric = metric_terms.reshape(3, 3, elements_here) * growth[None, None, :]
    physical = jnp.einsum("ide,dcne->icne", metric, slopes, precision=lax.Precision.HIGHEST)
    absorb = damping * absorb_mask.astype(jnp.float32)
    diverge = physical[0, 1] + physical[1, 2] + physical[2, 3]
    volume = jnp.concatenate([-diverge[None], -physical[:, 0]], 0)
    change = volume + lifted - absorb[None, None, :] * fields
    store_next = RUNGE_CARRY * section_store + TIME_STEP * change
    fields_next = fields + RUNGE_ADVANCE * store_next
    energy = jnp.sum(absorb * jnp.sum(fields_next * fields_next, (0, 1)))
    return fields_next, store_next, energy


def reference(fields, section_store, metric_terms, normals, face_scale, damping, absorb_mask, refine_level,
              face_source, orientation, derivative, lift_matrix):
    face_index, turn_index = node_tables()
    devices = N_GRP * N_SUB
    per_device = LOCAL_ELEMENTS
    slot_width = PEER_SLOTS
    box_size = (N_SUB + 2) * slot_width
    traces = fields[:, face_index, :]
    own_cols = jnp.transpose(traces.reshape(4, 4, FACE_NODES, devices, per_device), (0, 2, 3, 1, 4))
    own_cols = own_cols.reshape(4 * FACE_NODES, 4 * ELEMENTS)
    element = jnp.arange(ELEMENTS, dtype=jnp.int32)
    device = jnp.broadcast_to((element // per_device)[None, :], (4, ELEMENTS))
    within = jnp.broadcast_to((element % per_device)[None, :], (4, ELEMENTS))
    facet = jnp.arange(4, dtype=jnp.int32)[:, None]
    column = device * (4 * per_device) + facet * per_device + within
    face_codes = face_source
    is_local = (face_codes >= 0) & (face_codes < 4 * per_device)
    is_remote = face_codes >= 4 * per_device
    local_col = device * (4 * per_device) + jnp.clip(face_codes, 0, 4 * per_device - 1)
    slot_index = jnp.where(is_remote, face_codes - 4 * per_device, 0)
    block_index = slot_index // slot_width
    rank = slot_index % slot_width
    group_index = device // N_SUB
    member = device % N_SUB
    peer_dev = jnp.where(block_index < N_SUB, group_index * N_SUB + block_index,
                         jnp.where(block_index == N_SUB, device - N_SUB, device + N_SUB))
    peer_slot = jnp.where(block_index < N_SUB, member * slot_width + rank,
                          jnp.where(block_index == N_SUB, (N_SUB + 1) * slot_width + rank, N_SUB * slot_width + rank))
    owner_place = jnp.where(is_remote, device * box_size + slot_index, devices * box_size).astype(jnp.int32)
    slot_owner = jnp.zeros((devices * box_size,), jnp.int32).at[owner_place.reshape(-1)].set(
        column.reshape(-1), mode="drop")
    remote_col = slot_owner[jnp.clip(peer_dev * box_size + peer_slot, 0, devices * box_size - 1).astype(jnp.int32)]
    partner = jnp.where(is_local, local_col, jnp.where(is_remote, remote_col, 0)).astype(jnp.int32)

    def by_device(array):
        return jnp.transpose(array.reshape(array.shape[:-1] + (devices, per_device)),
                             (array.ndim - 1,) + tuple(range(array.ndim - 1)) + (array.ndim,))

    fields_d = by_device(fields)
    store_d = by_device(section_store)
    metric_d = by_device(metric_terms)
    normals_d = by_device(normals)
    scale_d = by_device(face_scale)
    damping_d = damping.reshape(devices, per_device)
    mask_d = absorb_mask.reshape(devices, per_device)
    level_d = refine_level.reshape(devices, per_device)
    codes_d = by_device(face_source).reshape(devices, 4 * per_device)
    orient_d = by_device(orientation).reshape(devices, 4 * per_device)
    partner_d = by_device(partner).reshape(devices, 4 * per_device)
    inner_d = jnp.transpose(own_cols.reshape(4 * FACE_NODES, devices, 4 * per_device), (1, 0, 2))

    def one_device(pieces):
        (fields_p, store_p, metric_p, normals_p, scale_p, damping_p, mask_p, level_p,
         codes_p, orient_p, inner_p, partner_p) = pieces
        outer_p = jnp.take(own_cols, partner_p, axis=1)
        return advance(fields_p, store_p, metric_p, normals_p, scale_p, damping_p, mask_p, level_p,
                       codes_p, orient_p, inner_p, outer_p, derivative, lift_matrix)

    fields_out, store_out, energies = lax.map(one_device, (fields_d, store_d, metric_d, normals_d, scale_d,
                                                          damping_d, mask_d, level_d, codes_d, orient_d,
                                                          inner_d, partner_d))
    fields_next = jnp.transpose(fields_out, (1, 2, 0, 3)).reshape(4, VOLUME_NODES, ELEMENTS)
    store_next = jnp.transpose(store_out, (1, 2, 0, 3)).reshape(4, VOLUME_NODES, ELEMENTS)
    absorbed_energy = jnp.sum(energies) / (ELEMENTS * VOLUME_NODES)
    return (fields_next, store_next, absorbed_energy)
```

```python
import jax
import jax.numpy as jnp
import numpy as np
from jax import lax
from jax.experimental import pallas as pl
from jax.experimental.pallas import tpu as pltpu
from jax.sharding import PartitionSpec as P

VOLUME_NODES = 35
FACE_NODES = 15
ROWS = 16

RUNGE_CARRY = -567301805773.0 / 1357537059087.0
RUNGE_ADVANCE = 5161836677717.0 / 13612068292357.0
TIME_STEP = 0.02
INVERSE_TURN = (0, 2, 1, 3, 4, 5)


def node_tables():
    volume_list = [
        (a, b, c, 4 - a - b - c)
        for a in range(5)
        for b in range(5 - a)
        for c in range(5 - a - b)
    ]
    triples = [(a, b, 4 - a - b) for a in range(5) for b in range(5 - a)]
    face_index = np.zeros((4, 15), np.int32)
    for facet in range(4):
        others = [corner for corner in range(4) if corner != facet]
        for node_pos in range(15):
            corners = [0, 0, 0, 0]
            for place_pos in range(3):
                corners[others[place_pos]] = triples[node_pos][place_pos]
            face_index[facet, node_pos] = volume_list.index(tuple(corners))
    vertex_orders = [(0, 1, 2), (1, 2, 0), (2, 0, 1), (0, 2, 1), (2, 1, 0), (1, 0, 2)]
    turn_index = np.zeros((6, 15), np.int32)
    for option in range(6):
        order = vertex_orders[option]
        for node_pos in range(15):
            triple = triples[node_pos]
            turned = (triple[order[0]], triple[order[1]], triple[order[2]])
            turn_index[option, node_pos] = triples.index(turned)
    return face_index, turn_index


FACE_INDEX, TURN_INDEX = node_tables()


def split_three(value):
    high = value.astype(jnp.bfloat16)
    rest = value - high.astype(jnp.float32)
    middle = rest.astype(jnp.bfloat16)
    low = (rest - middle.astype(jnp.float32)).astype(jnp.bfloat16)
    return high, middle, low


def turned_traces(fields_ref, orient_ref, turned_ref, elements_here):
    for facet in range(4):
        for start in range(0, elements_here, 128):
            lanes = slice(start, start + 128)
            tile = (facet * elements_here + start) // 128
            own_turn = jnp.broadcast_to(orient_ref[facet : facet + 1, lanes], (4, 128))
            is_turn = [own_turn == option for option in range(6)]
            nodes = [fields_ref[int(FACE_INDEX[facet, j]), :, lanes] for j in range(FACE_NODES)]
            for j in range(FACE_NODES):
                by_source = {}
                for option in range(6):
                    source = int(TURN_INDEX[INVERSE_TURN[option], j])
                    by_source.setdefault(source, []).append(option)
                items = list(by_source.items())
                value = nodes[items[0][0]]
                for source, options in items[1:]:
                    mask = is_turn[options[0]]
                    for option in options[1:]:
                        mask = mask | is_turn[option]
                    value = jnp.where(mask, nodes[source], value)
                turned_ref[tile, pl.ds(j, 4, stride=ROWS), :] = value
            turned_ref[tile, pl.ds(15, 4, stride=ROWS), :] = jnp.zeros((4, 128), jnp.float32)


def side_by_side(tiles_ref):
    return jnp.concatenate([tiles_ref[tile] for tile in range(tiles_ref.shape[0])], 1)


def code_row(code_ref, facet):
    return code_ref[facet : facet + 1, :]


def slot_hits(code_ref, slots, total_faces):
    parts = []
    for facet in range(4):
        codes = code_row(code_ref, facet) - total_faces
        rows = lax.broadcasted_iota(jnp.int32, (slots, codes.shape[1]), 0)
        parts.append(jnp.where(rows == codes, 1.0, 0.0).astype(jnp.bfloat16))
    return jnp.concatenate(parts, 1)


def pack_kernel(peers, fields_ref, code_ref, orient_ref, near_ref, up_ref, down_ref, turned_ref):
    elements_here = fields_ref.shape[2]
    total_faces = 4 * elements_here
    width = elements_here // 8
    blocks = peers + 2
    turned_traces(fields_ref, orient_ref, turned_ref, elements_here)
    parts = jnp.concatenate(split_three(side_by_side(turned_ref)), 0)
    hits = slot_hits(code_ref, blocks * width, total_faces)
    packed = lax.dot_general(
        parts, hits, (((1,), (1,)), ((), ())), preferred_element_type=jnp.float32
    )
    rows = 4 * ROWS
    packed = packed[:rows] + (packed[rows : 2 * rows] + packed[2 * rows :])
    for block in range(blocks):
        columns = slice(block * width, (block + 1) * width)
        value = jnp.concatenate(
            [packed[c * ROWS : (c + 1) * ROWS, columns] for c in range(4)], 1
        )
        if block < peers:
            near_ref[block] = value
        elif block == peers:
            down_ref[...] = value
        else:
            up_ref[...] = value


def inner_kernel(
    fields_ref,
    store_ref,
    metric_ref,
    normal_ref,
    scale_ref,
    damping_ref,
    mask_ref,
    level_ref,
    code_ref,
    orient_ref,
    derivative_ref,
    lift_ref,
    base_ref,
    plain_ref,
    flux_ref,
    weight_ref,
    absorb_ref,
    lift_out_ref,
    turned_ref,
    trace_ref,
):
    elements_here = fields_ref.shape[2]
    total_faces = 4 * elements_here
    growth = jnp.exp2(level_ref[...].astype(jnp.float32))
    absorb = damping_ref[...] * mask_ref[...].astype(jnp.float32)
    absorb_ref[...] = absorb
    weight_ref[...] = 0.5 * (scale_ref[...] * growth)
    plain = [fields_ref[:, c, :] for c in range(4)]
    for c in range(4):
        plain_ref[c] = plain[c]
    joined = jnp.concatenate(plain, 1)
    slopes = [
        jnp.dot(
            derivative_ref[y],
            joined,
            precision=lax.Precision.HIGHEST,
            preferred_element_type=jnp.float32,
        )
        for y in range(3)
    ]

    def slope(y, c):
        return slopes[y][:, c * elements_here : (c + 1) * elements_here]

    metric = metric_ref[...] * growth

    def physical(x, c):
        total = metric[3 * x : 3 * x + 1] * slope(0, c)
        for y in (1, 2):
            total = total + metric[3 * x + y : 3 * x + y + 1] * slope(y, c)
        return total

    for c in range(4):
        if c == 0:
            volume = physical(0, 1) + physical(1, 2) + physical(2, 3)
        else:
            volume = physical(c - 1, 0)
        change = -volume - absorb * plain[c]
        base_ref[c] = RUNGE_CARRY * store_ref[:, c, :] + TIME_STEP * change
    for facet in range(4):
        for tile in range(elements_here // 128):
            for j in range(ROWS):
                if j < FACE_NODES:
                    node = int(FACE_INDEX[facet, j])
                    value = fields_ref[node, :, tile * 128 : tile * 128 + 128]
                else:
                    value = jnp.zeros((4, 128), jnp.float32)
                trace_ref[tile, pl.ds(facet * ROWS + j, 4, stride=4 * ROWS), :] = value
    traces = side_by_side(trace_ref)
    turned_traces(fields_ref, orient_ref, turned_ref, elements_here)
    parts = jnp.concatenate(split_three(side_by_side(turned_ref)), 0)
    rows = 4 * ROWS
    for facet in range(4):
        codes = code_row(code_ref, facet)
        hits = jnp.where(
            lax.broadcasted_iota(jnp.int32, (total_faces, elements_here), 0) == codes, 1.0, 0.0
        ).astype(jnp.bfloat16)
        found = jnp.dot(parts, hits, preferred_element_type=jnp.float32)
        found = found[:rows] + (found[rows : 2 * rows] + found[2 * rows :])
        inside = [
            traces[c * rows + facet * ROWS : c * rows + facet * ROWS + ROWS] for c in range(4)
        ]
        outside = [found[c * ROWS : (c + 1) * ROWS] for c in range(4)]
        normal = [normal_ref[x, facet : facet + 1, :] for x in range(3)]
        wall = codes < 0
        normal_in = normal[0] * inside[1] + normal[1] * inside[2] + normal[2] * inside[3]
        press_jump = jnp.where(wall, 0.0, inside[0] - outside[0])
        normal_jump = jnp.zeros_like(press_jump)
        for x in range(3):
            step = jnp.where(
                wall, 2.0 * normal[x] * normal_in, inside[1 + x] - outside[1 + x]
            )
            normal_jump = normal_jump + normal[x] * step
        weight = 0.5 * (scale_ref[facet : facet + 1, :] * growth)
        flux_ref[facet * ROWS : (facet + 1) * ROWS, :] = weight * (normal_jump - press_jump)
    wide = lax.broadcasted_iota(jnp.int32, (4 * FACE_NODES, rows), 1)
    tall = lax.broadcasted_iota(jnp.int32, (4 * FACE_NODES, rows), 0)
    facet_of = wide // ROWS
    place = jnp.where(
        (tall == wide - facet_of) & (wide - facet_of * ROWS < FACE_NODES), 1.0, 0.0
    )
    spread = jnp.dot(
        lift_ref[...],
        place,
        precision=lax.Precision.HIGHEST,
        preferred_element_type=jnp.float32,
    )
    high, middle, low = split_three(spread)
    lift_out_ref[...] = jnp.concatenate([high, high, middle, middle], 1)


def outer_kernel(
    peers,
    near_ref,
    below_ref,
    above_ref,
    code_ref,
    normal_ref,
    weight_ref,
    flux_ref,
    lift_ref,
    base_ref,
    plain_ref,
    absorb_ref,
    fields_ref,
    store_ref,
    energy_ref,
):
    elements_here = plain_ref.shape[2]
    total_faces = 4 * elements_here
    width = elements_here // 8
    blocks = peers + 2
    rows = 4 * ROWS
    boxes = [near_ref[block] for block in range(peers)] + [below_ref[...], above_ref[...]]
    received = jnp.concatenate(
        [
            jnp.concatenate([box[:, c * width : (c + 1) * width] for box in boxes], 1)
            for c in range(4)
        ],
        0,
    )
    parts = jnp.concatenate(split_three(received), 0)
    hits = slot_hits(code_ref, blocks * width, total_faces)
    found = jnp.dot(parts, hits, preferred_element_type=jnp.float32)
    found = found[:rows] + (found[rows : 2 * rows] + found[2 * rows :])
    pieces = []
    for facet in range(4):
        columns = slice(facet * elements_here, (facet + 1) * elements_here)
        outside = [found[c * ROWS : (c + 1) * ROWS, columns] for c in range(4)]
        normal = [normal_ref[x, facet : facet + 1, :] for x in range(3)]
        across = normal[0] * outside[1] + normal[1] * outside[2] + normal[2] * outside[3]
        weight = weight_ref[facet : facet + 1, :]
        press = flux_ref[facet * ROWS : (facet + 1) * ROWS, :] + weight * (outside[0] - across)
        pieces.append([press] + [-normal[x] * press for x in range(3)])
    flux = jnp.concatenate(
        [jnp.concatenate([pieces[facet][c] for facet in range(4)], 0) for c in range(4)], 1
    )
    high = flux.astype(jnp.bfloat16)
    middle = (flux - high.astype(jnp.float32)).astype(jnp.bfloat16)
    lifted = jnp.dot(
        lift_ref[...],
        jnp.concatenate([high, middle, high, middle], 0),
        preferred_element_type=jnp.float32,
    )
    square = jnp.zeros((VOLUME_NODES, elements_here), jnp.float32)
    for c in range(4):
        columns = slice(c * elements_here, (c + 1) * elements_here)
        store_next = base_ref[c] + TIME_STEP * lifted[:, columns]
        fields_next = plain_ref[c] + RUNGE_ADVANCE * store_next
        store_ref[:, c, :] = store_next
        fields_ref[:, c, :] = fields_next
        square = square + fields_next * fields_next
    energy = jnp.sum(square, 0, keepdims=True) * absorb_ref[...]
    total = energy[:, :128]
    for start in range(128, elements_here, 128):
        total = total + energy[:, start : start + 128]
    energy_ref[...] = jnp.broadcast_to(total[None], energy_ref.shape)


def local(
    fields,
    section_store,
    metric_terms,
    normals,
    face_scale,
    damping,
    absorb_mask,
    refine_level,
    face_source,
    orientation,
    derivative,
    lift_matrix,
):
    elements_here = fields.shape[2]
    total_faces = 4 * elements_here
    peers = lax.axis_size("sub")
    slabs = lax.axis_size("grp")
    devices = peers * slabs
    f32 = jnp.float32
    fields_t = jnp.transpose(fields, (1, 0, 2))
    store_t = jnp.transpose(section_store, (1, 0, 2))
    normals_t = jnp.transpose(normals, (1, 0, 2))
    row = (1, elements_here)
    near, up, down = pl.pallas_call(
        lambda *refs: pack_kernel(peers, *refs),
        out_shape=(
            jax.ShapeDtypeStruct((peers, ROWS, 128), f32),
            jax.ShapeDtypeStruct((ROWS, 128), f32),
            jax.ShapeDtypeStruct((ROWS, 128), f32),
        ),
        scratch_shapes=[pltpu.VMEM((total_faces // 128, 4 * ROWS, 128), f32)],
        name="pack",
    )(fields_t, face_source, orientation)
    arrived = lax.all_to_all(near, "sub", split_axis=0, concat_axis=0, tiled=True)
    from_below = lax.ppermute(up, "grp", [(g, g + 1) for g in range(slabs - 1)])
    from_above = lax.ppermute(down, "grp", [(g + 1, g) for g in range(slabs - 1)])
    base, plain, flux, weight, absorb, lift_parts = pl.pallas_call(
        inner_kernel,
        out_shape=(
            jax.ShapeDtypeStruct((4, VOLUME_NODES, elements_here), f32),
            jax.ShapeDtypeStruct((4, VOLUME_NODES, elements_here), f32),
            jax.ShapeDtypeStruct((4 * ROWS, elements_here), f32),
            jax.ShapeDtypeStruct((4, elements_here), f32),
            jax.ShapeDtypeStruct(row, f32),
            jax.ShapeDtypeStruct((VOLUME_NODES, 16 * ROWS), jnp.bfloat16),
        ),
        scratch_shapes=[
            pltpu.VMEM((total_faces // 128, 4 * ROWS, 128), f32),
            pltpu.VMEM((elements_here // 128, 16 * ROWS, 128), f32),
        ],
        name="inner",
    )(
        fields_t,
        store_t,
        metric_terms,
        normals_t,
        face_scale,
        damping.reshape(row),
        absorb_mask.reshape(row),
        refine_level.reshape(row),
        face_source,
        orientation,
        derivative,
        lift_matrix,
    )
    fields_next, store_next, energy = pl.pallas_call(
        lambda *refs: outer_kernel(peers, *refs),
        out_shape=(
            jax.ShapeDtypeStruct((VOLUME_NODES, 4, elements_here), f32),
            jax.ShapeDtypeStruct((VOLUME_NODES, 4, elements_here), f32),
            jax.ShapeDtypeStruct((devices, 1, 128), f32),
        ),
        name="outer",
    )(
        arrived,
        from_below,
        from_above,
        face_source,
        normals_t,
        weight,
        flux,
        lift_parts,
        base,
        plain,
        absorb,
    )
    shares = lax.all_to_all(energy, ("grp", "sub"), split_axis=0, concat_axis=0, tiled=True)
    divisor = elements_here * devices * VOLUME_NODES
    return (
        jnp.transpose(fields_next, (1, 0, 2)),
        jnp.transpose(store_next, (1, 0, 2)),
        jnp.sum(shares) / divisor,
    )


def solution(mesh):
    placed = (
        P(None, None, ("grp", "sub")),
        P(None, None, ("grp", "sub")),
        P(None, ("grp", "sub")),
        P(None, None, ("grp", "sub")),
        P(None, ("grp", "sub")),
        P(("grp", "sub")),
        P(("grp", "sub")),
        P(("grp", "sub")),
        P(None, ("grp", "sub")),
        P(None, ("grp", "sub")),
        P(),
        P(),
    )
    return jax.shard_map(
        local,
        mesh=mesh,
        in_specs=placed,
        out_specs=(P(None, None, ("grp", "sub")), P(None, None, ("grp", "sub")), P()),
        check_vma=False,
    )
```

```python
import jax
import jax.numpy as jnp
import numpy as np
from jax import lax
from jax.experimental import pallas as pl
from jax.experimental.pallas import tpu as pltpu
from jax.sharding import PartitionSpec as P


VOLUME_NODES = 35
FACE_NODES = 15
ROWS = 16
PITCH = 24
TRACE_PITCH = 72

RUNGE_CARRY = -567301805773.0 / 1357537059087.0
RUNGE_ADVANCE = 5161836677717.0 / 13612068292357.0
TIME_STEP = 0.02
INVERSE_TURN = (0, 2, 1, 3, 4, 5)


def node_tables():
    volume_list = [
        (a, b, c, 4 - a - b - c)
        for a in range(5)
        for b in range(5 - a)
        for c in range(5 - a - b)
    ]
    triples = [(a, b, 4 - a - b) for a in range(5) for b in range(5 - a)]
    face_index = np.zeros((4, 15), np.int32)
    for facet in range(4):
        others = [corner for corner in range(4) if corner != facet]
        for node_pos in range(15):
            corners = [0, 0, 0, 0]
            for place_pos in range(3):
                corners[others[place_pos]] = triples[node_pos][place_pos]
            face_index[facet, node_pos] = volume_list.index(tuple(corners))
    vertex_orders = [(0, 1, 2), (1, 2, 0), (2, 0, 1), (0, 2, 1), (2, 1, 0), (1, 0, 2)]
    turn_index = np.zeros((6, 15), np.int32)
    for option in range(6):
        order = vertex_orders[option]
        for node_pos in range(15):
            triple = triples[node_pos]
            turned = (triple[order[0]], triple[order[1]], triple[order[2]])
            turn_index[option, node_pos] = triples.index(turned)
    return face_index, turn_index


FACE_INDEX, TURN_INDEX = node_tables()


def split_three(value):
    high = value.astype(jnp.bfloat16)
    rest = value - high.astype(jnp.float32)
    middle = rest.astype(jnp.bfloat16)
    low = (rest - middle.astype(jnp.float32)).astype(jnp.bfloat16)
    return high, middle, low


def select_turn(nodes, is_turn, j):
    by_source = {}
    for option in range(6):
        source = int(TURN_INDEX[INVERSE_TURN[option], j])
        by_source.setdefault(source, []).append(option)
    items = list(by_source.items())
    value = nodes[items[0][0]]
    for source, options in items[1:]:
        mask = is_turn[options[0]]
        for option in options[1:]:
            mask = mask | is_turn[option]
        value = jnp.where(mask, nodes[source], value)
    return value


def lane_halves(ref, row):
    halves = [jnp.broadcast_to(ref[row : row + 1, h * 128 : h * 128 + 128], (4, 128)) for h in (0, 1)]
    return jnp.concatenate(halves, 0)


def add_parts(value):
    rows = value.shape[0] // 3
    return value[:rows] + (value[rows : 2 * rows] + value[2 * rows :])


def mark_hits(code_ref, hits_ref):
    elements_here = code_ref.shape[1]
    for facet in range(4):
        codes = code_ref[facet : facet + 1, :] - 4 * elements_here
        rows = lax.broadcasted_iota(jnp.int32, (hits_ref.shape[0], elements_here), 0)
        hits_ref[:, facet * elements_here : (facet + 1) * elements_here] = jnp.where(
            rows == codes, 1.0, 0.0
        ).astype(jnp.bfloat16)


def pack_kernel(peers, count, *refs):
    source = refs[:count]
    near_ref, up_ref, down_ref, parts_ref = refs[2 * count - 1 : 2 * count + 3]
    hits_ref, orient_ref, turned_ref, box_ref, sems, box_sem = refs[2 * count + 3 :]
    target = (refs[count], orient_ref) + refs[count + 1 : 2 * count - 1]
    copies = [pltpu.make_async_copy(source[i], target[i], sems.at[i]) for i in range(count)]
    for copy in copies:
        copy.start()
    code_ref, fields_ref = target[0], target[2]
    elements_here = code_ref.shape[1]
    width = elements_here // 8
    blocks = peers + 2
    copies[0].wait()
    mark_hits(code_ref, hits_ref)
    copies[1].wait()
    copies[2].wait()
    for facet in range(4):
        own_turn = lane_halves(orient_ref, facet)
        is_turn = [own_turn == option for option in range(6)]
        nodes = []
        for j in range(FACE_NODES):
            node = int(FACE_INDEX[facet, j])
            nodes.append(fields_ref[node * 8 : node * 8 + 8, :])
        for j in range(ROWS):
            if j < FACE_NODES:
                value = select_turn(nodes, is_turn, j)
            else:
                value = jnp.zeros((8, 128), jnp.float32)
            turned_ref[facet, pl.ds(j, 8, stride=PITCH), :] = value
    turned = jnp.concatenate(
        [
            jnp.concatenate(
                [turned_ref[f, (h * 4 + c) * PITCH : (h * 4 + c) * PITCH + ROWS, :] for c in range(4)], 0
            )
            for f in range(4)
            for h in range(2)
        ],
        1,
    )
    parts = jnp.concatenate(split_three(turned), 0)
    parts_ref[...] = parts
    packed = add_parts(
        lax.dot_general(
            parts, hits_ref[...], (((1,), (1,)), ((), ())), preferred_element_type=jnp.float32
        )
    )
    for block in range(blocks):
        columns = slice(block * width, (block + 1) * width)
        value = jnp.concatenate(
            [packed[c * ROWS : (c + 1) * ROWS, columns] for c in range(4)], 1
        )
        if block < peers:
            box_ref[block] = value
        elif block == peers:
            down_ref[...] = value
        else:
            up_ref[...] = value
    out = pltpu.make_async_copy(box_ref, near_ref, box_sem)
    out.start()
    for copy in copies[3:]:
        copy.wait()
    out.wait()


def inner_kernel(
    code_ref,
    fields_ref,
    store_ref,
    metric_ref,
    normal_ref,
    scale_ref,
    damping_ref,
    mask_ref,
    level_ref,
    derivative_ref,
    lift_ref,
    parts_ref,
    base_ref,
    plain_ref,
    flux_ref,
    weight_ref,
    absorb_ref,
    lift_out_ref,
    trace_ref,
):
    elements_here = code_ref.shape[1]
    total_faces = 4 * elements_here
    growth = jnp.exp2(level_ref[...].astype(jnp.float32))
    absorb = damping_ref[...] * mask_ref[...].astype(jnp.float32)
    absorb_ref[...] = absorb
    weight = 0.5 * (scale_ref[...] * growth)
    weight_ref[...] = weight

    def by_field(ref, c):
        return jnp.concatenate(
            [ref[pl.ds(h * 4 + c, VOLUME_NODES, stride=8), :] for h in range(2)], 1
        )

    for facet in range(4):
        for j in range(ROWS):
            if j < FACE_NODES:
                node = int(FACE_INDEX[facet, j])
                value = fields_ref[node * 8 : node * 8 + 8, :]
            else:
                value = jnp.zeros((8, 128), jnp.float32)
            trace_ref[pl.ds(facet * ROWS + j, 8, stride=TRACE_PITCH), :] = value
    parts = parts_ref[...]
    for facet in range(4):
        codes = code_ref[facet : facet + 1, :]
        hits = jnp.where(
            lax.broadcasted_iota(jnp.int32, (total_faces, elements_here), 0) == codes, 1.0, 0.0
        ).astype(jnp.bfloat16)
        found = add_parts(jnp.dot(parts, hits, preferred_element_type=jnp.float32))
        inside = []
        for c in range(4):
            starts = [(h * 4 + c) * TRACE_PITCH + facet * ROWS for h in range(2)]
            inside.append(jnp.concatenate([trace_ref[a : a + ROWS, :] for a in starts], 1))
        outside = [found[c * ROWS : (c + 1) * ROWS] for c in range(4)]
        normal = [normal_ref[x, facet : facet + 1, :] for x in range(3)]
        wall = codes < 0
        normal_in = normal[0] * inside[1] + normal[1] * inside[2] + normal[2] * inside[3]
        press_jump = jnp.where(wall, 0.0, inside[0] - outside[0])
        normal_jump = jnp.zeros_like(press_jump)
        for x in range(3):
            step = jnp.where(wall, 2.0 * normal[x] * normal_in, inside[1 + x] - outside[1 + x])
            normal_jump = normal_jump + normal[x] * step
        flux_ref[facet * ROWS : (facet + 1) * ROWS, :] = weight[facet : facet + 1] * (
            normal_jump - press_jump
        )
    plain = [by_field(fields_ref, c) for c in range(4)]
    for c in range(4):
        plain_ref[c] = plain[c]
    joined = jnp.concatenate(plain, 1)
    padded = jnp.concatenate([joined, jnp.zeros((5, joined.shape[1]), jnp.float32)], 0)
    high = padded.astype(jnp.bfloat16).astype(jnp.float32)
    stacked = jnp.concatenate([high, padded - high, high], 0).astype(jnp.bfloat16)
    slopes = []
    gap = jnp.zeros((VOLUME_NODES, 5), jnp.float32)
    for y in range(3):
        whole = derivative_ref[y]
        lead = whole.astype(jnp.bfloat16).astype(jnp.float32)
        left = jnp.concatenate([lead, gap, lead, gap, whole - lead, gap], 1).astype(jnp.bfloat16)
        slopes.append(jnp.dot(left, stacked, preferred_element_type=jnp.float32))

    def slope(y, c):
        return slopes[y][:, c * elements_here : (c + 1) * elements_here]

    metric = metric_ref[...] * growth

    def physical(x, c):
        total = metric[3 * x : 3 * x + 1] * slope(0, c)
        for y in (1, 2):
            total = total + metric[3 * x + y : 3 * x + y + 1] * slope(y, c)
        return total

    for c in range(4):
        if c == 0:
            volume = physical(0, 1) + physical(1, 2) + physical(2, 3)
        else:
            volume = physical(c - 1, 0)
        change = -volume - absorb * plain[c]
        base_ref[c] = RUNGE_CARRY * by_field(store_ref, c) + TIME_STEP * change
    none = jnp.zeros((VOLUME_NODES, 1), jnp.float32)
    pieces = []
    for facet in range(4):
        pieces += [lift_ref[:, facet * FACE_NODES : (facet + 1) * FACE_NODES], none]
    high, middle, _ = split_three(jnp.concatenate(pieces, 1))
    lift_out_ref[...] = jnp.concatenate([high, high, middle, middle], 1)


def outer_kernel(
    peers,
    hold_hits,
    near_ref,
    below_ref,
    above_ref,
    hits_ref,
    normal_ref,
    weight_ref,
    flux_ref,
    lift_ref,
    base_ref,
    plain_ref,
    absorb_ref,
    fields_ref,
    store_ref,
    energy_ref,
    *scratch,
):
    elements_here = plain_ref.shape[2]
    width = elements_here // 8
    if not hold_hits:
        mark_hits(hits_ref, scratch[0])
        hits_ref = scratch[0]
    boxes = [near_ref[block] for block in range(peers)] + [below_ref[...], above_ref[...]]
    received = jnp.concatenate(
        [
            jnp.concatenate([box[:, c * width : (c + 1) * width] for box in boxes], 1)
            for c in range(4)
        ],
        0,
    )
    parts = jnp.concatenate(split_three(received), 0)
    found = add_parts(jnp.dot(parts, hits_ref[...], preferred_element_type=jnp.float32))
    pieces = []
    for facet in range(4):
        columns = slice(facet * elements_here, (facet + 1) * elements_here)
        outside = [found[c * ROWS : (c + 1) * ROWS, columns] for c in range(4)]
        normal = [normal_ref[x, facet : facet + 1, :] for x in range(3)]
        across = normal[0] * outside[1] + normal[1] * outside[2] + normal[2] * outside[3]
        weight = weight_ref[facet : facet + 1, :]
        press = flux_ref[facet * ROWS : (facet + 1) * ROWS, :] + weight * (outside[0] - across)
        pieces.append([press] + [-normal[x] * press for x in range(3)])
    flux = jnp.concatenate(
        [jnp.concatenate([pieces[facet][c] for facet in range(4)], 0) for c in range(4)], 1
    )
    high = flux.astype(jnp.bfloat16)
    middle = (flux - high.astype(jnp.float32)).astype(jnp.bfloat16)
    lifted = jnp.dot(
        lift_ref[...],
        jnp.concatenate([high, middle, high, middle], 0),
        preferred_element_type=jnp.float32,
    )
    square = jnp.zeros((VOLUME_NODES, elements_here), jnp.float32)
    for c in range(4):
        columns = slice(c * elements_here, (c + 1) * elements_here)
        store_next = base_ref[c] + TIME_STEP * lifted[:, columns]
        fields_next = plain_ref[c] + RUNGE_ADVANCE * store_next
        for h in range(2):
            lanes = slice(h * 128, h * 128 + 128)
            store_ref[pl.ds(h * 4 + c, VOLUME_NODES, stride=8), :] = store_next[:, lanes]
            fields_ref[pl.ds(h * 4 + c, VOLUME_NODES, stride=8), :] = fields_next[:, lanes]
        square = square + fields_next * fields_next
    energy = jnp.sum(square, 0, keepdims=True) * absorb_ref[...]
    total = energy[:, :128] + energy[:, 128:]
    energy_ref[...] = jnp.broadcast_to(total[None], energy_ref.shape)


def finish_kernel(divisor, shares_ref, fields_in, store_in, total_ref, fields_out, store_out, sems):
    one = pltpu.make_async_copy(fields_in, fields_out, sems.at[0])
    two = pltpu.make_async_copy(store_in, store_out, sems.at[1])
    one.start()
    two.start()
    total_ref[0] = jnp.sum(shares_ref[...]) * (1.0 / divisor)
    one.wait()
    two.wait()


def as_rows(value):
    fields, nodes, elements = value.shape
    value = jnp.transpose(value.reshape(fields, nodes, elements // 128, 128), (1, 2, 0, 3))
    return value.reshape(nodes * 8, 128)


def from_rows(value, nodes):
    value = jnp.transpose(value.reshape(nodes, 2, 4, 128), (2, 0, 1, 3))
    return value.reshape(4, nodes, 256)


def in_vmem(*values):
    return [pltpu.with_memory_space_constraint(value, pltpu.VMEM) for value in values]


def local(
    fields,
    section_store,
    metric_terms,
    normals,
    face_scale,
    damping,
    absorb_mask,
    refine_level,
    face_source,
    orientation,
    derivative,
    lift_matrix,
):
    elements_here = fields.shape[2]
    assert elements_here == 256
    total_faces = 4 * elements_here
    peers = lax.axis_size("sub")
    slabs = lax.axis_size("grp")
    devices = peers * slabs
    slots = (peers + 2) * (elements_here // 8)
    f32 = jnp.float32
    bf16 = jnp.bfloat16
    hits_shape = pltpu.VMEM((slots, total_faces), bf16)
    hold_hits = 2 * slots * total_faces <= 2**20
    row = (1, elements_here)
    given = [
        face_source,
        orientation,
        as_rows(fields),
        as_rows(section_store),
        metric_terms,
        jnp.transpose(normals, (1, 0, 2)),
        face_scale,
        damping.reshape(row),
        absorb_mask.reshape(row),
        refine_level.reshape(row),
        derivative,
        lift_matrix,
    ]
    count = len(given)
    kept = given[:1] + given[2:]
    packed = pl.pallas_call(
        lambda *refs: pack_kernel(peers, count, *refs),
        out_shape=tuple(pltpu.VMEM(value.shape, value.dtype) for value in kept)
        + (
            jax.ShapeDtypeStruct((peers, ROWS, 128), f32),
            pltpu.VMEM((ROWS, 128), f32),
            pltpu.VMEM((ROWS, 128), f32),
            pltpu.VMEM((12 * ROWS, total_faces), bf16),
        )
        + ((hits_shape,) if hold_hits else ()),
        in_specs=[pl.BlockSpec(memory_space=pltpu.HBM)] * count,
        out_specs=tuple([pl.BlockSpec(memory_space=pltpu.VMEM)] * len(kept))
        + (pl.BlockSpec(memory_space=pltpu.HBM),)
        + tuple([pl.BlockSpec(memory_space=pltpu.VMEM)] * (4 if hold_hits else 3)),
        scratch_shapes=([] if hold_hits else [hits_shape])
        + [
            pltpu.VMEM((4, elements_here), jnp.int32),
            pltpu.VMEM((4, 8 * PITCH, 128), f32),
            pltpu.VMEM((peers, ROWS, 128), f32),
            pltpu.SemaphoreType.DMA((count,)),
            pltpu.SemaphoreType.DMA,
        ],
        name="pack",
    )(*given)
    held = packed[: len(kept)]
    near, up, down, parts = packed[len(kept) : len(kept) + 4]
    first = [(g, g + 1) for g in range(0, slabs - 1, 2)]
    second = [(g, g + 1) for g in range(1, slabs - 1, 2)]
    odd = lax.axis_index("grp") % 2 == 1
    arrived = lax.all_to_all(near, "sub", split_axis=0, concat_axis=0, tiled=True)
    swap_a = lax.ppermute(jnp.where(odd, down, up), "grp", first + [(b, a) for a, b in first])
    swap_b = lax.ppermute(jnp.where(odd, up, down), "grp", second + [(b, a) for a, b in second])
    from_below = jnp.where(odd, swap_a, swap_b)
    from_above = jnp.where(odd, swap_b, swap_a)
    base, plain, flux, weight, absorb, lift_parts = pl.pallas_call(
        inner_kernel,
        out_shape=(
            pltpu.VMEM((4, VOLUME_NODES, elements_here), f32),
            pltpu.VMEM((4, VOLUME_NODES, elements_here), f32),
            pltpu.VMEM((4 * ROWS, elements_here), f32),
            pltpu.VMEM((4, elements_here), f32),
            pltpu.VMEM(row, f32),
            pltpu.VMEM((VOLUME_NODES, 16 * ROWS), bf16),
        ),
        scratch_shapes=[pltpu.VMEM((8 * TRACE_PITCH, 128), f32)],
        name="inner",
    )(*in_vmem(*held, parts))
    fields_next, store_next, energy = pl.pallas_call(
        lambda *refs: outer_kernel(peers, hold_hits, *refs),
        out_shape=(
            pltpu.VMEM((VOLUME_NODES * 8, 128), f32),
            pltpu.VMEM((VOLUME_NODES * 8, 128), f32),
            pltpu.VMEM((devices, 1, 128), f32),
        ),
        scratch_shapes=[] if hold_hits else [hits_shape],
        name="outer",
    )(
        *in_vmem(
            arrived,
            from_below,
            from_above,
            packed[-1] if hold_hits else held[0],
            held[4],
            weight,
            flux,
            lift_parts,
            base,
            plain,
            absorb,
        )
    )
    shares = lax.all_to_all(energy, ("grp", "sub"), split_axis=0, concat_axis=0, tiled=True)
    divisor = elements_here * devices * VOLUME_NODES
    total, fields_next, store_next = pl.pallas_call(
        lambda *refs: finish_kernel(divisor, *refs),
        out_shape=(
            jax.ShapeDtypeStruct((1,), f32),
            jax.ShapeDtypeStruct((VOLUME_NODES * 8, 128), f32),
            jax.ShapeDtypeStruct((VOLUME_NODES * 8, 128), f32),
        ),
        in_specs=[pl.BlockSpec(memory_space=pltpu.VMEM)] * 3,
        out_specs=(
            pl.BlockSpec(memory_space=pltpu.SMEM),
            pl.BlockSpec(memory_space=pltpu.HBM),
            pl.BlockSpec(memory_space=pltpu.HBM),
        ),
        scratch_shapes=[pltpu.SemaphoreType.DMA((2,))],
        name="finish",
    )(*in_vmem(shares, fields_next, store_next))
    return (
        from_rows(fields_next, VOLUME_NODES),
        from_rows(store_next, VOLUME_NODES),
        total[0],
    )


def solution(mesh):
    placed = (
        P(None, None, ("grp", "sub")),
        P(None, None, ("grp", "sub")),
        P(None, ("grp", "sub")),
        P(None, None, ("grp", "sub")),
        P(None, ("grp", "sub")),
        P(("grp", "sub")),
        P(("grp", "sub")),
        P(("grp", "sub")),
        P(None, ("grp", "sub")),
        P(None, ("grp", "sub")),
        P(),
        P(),
    )
    return jax.shard_map(
        local,
        mesh=mesh,
        in_specs=placed,
        out_specs=(P(None, None, ("grp", "sub")), P(None, None, ("grp", "sub")), P()),
        check_vma=False,
    )
```

```python
import jax
import jax.numpy as jnp
import numpy as np
from jax import lax
from jax.experimental import pallas as pl
from jax.experimental.pallas import tpu as pltpu
from jax.sharding import PartitionSpec as P


VOLUME_NODES = 35
FACE_NODES = 15
ROWS = 16
PITCH = 24
TRACE_PITCH = 72

RUNGE_CARRY = -567301805773.0 / 1357537059087.0
RUNGE_ADVANCE = 5161836677717.0 / 13612068292357.0
TIME_STEP = 0.02
INVERSE_TURN = (0, 2, 1, 3, 4, 5)


def node_tables():
    volume_list = [
        (a, b, c, 4 - a - b - c)
        for a in range(5)
        for b in range(5 - a)
        for c in range(5 - a - b)
    ]
    triples = [(a, b, 4 - a - b) for a in range(5) for b in range(5 - a)]
    face_index = np.zeros((4, 15), np.int32)
    for facet in range(4):
        others = [corner for corner in range(4) if corner != facet]
        for node_pos in range(15):
            corners = [0, 0, 0, 0]
            for place_pos in range(3):
                corners[others[place_pos]] = triples[node_pos][place_pos]
            face_index[facet, node_pos] = volume_list.index(tuple(corners))
    vertex_orders = [(0, 1, 2), (1, 2, 0), (2, 0, 1), (0, 2, 1), (2, 1, 0), (1, 0, 2)]
    turn_index = np.zeros((6, 15), np.int32)
    for option in range(6):
        order = vertex_orders[option]
        for node_pos in range(15):
            triple = triples[node_pos]
            turned = (triple[order[0]], triple[order[1]], triple[order[2]])
            turn_index[option, node_pos] = triples.index(turned)
    return face_index, turn_index


FACE_INDEX, TURN_INDEX = node_tables()


def split_two(value):
    high = value.astype(jnp.bfloat16)
    return high, (value - high.astype(jnp.float32)).astype(jnp.bfloat16)


def select_turn(nodes, is_turn, j):
    by_source = {}
    for option in range(6):
        source = int(TURN_INDEX[INVERSE_TURN[option], j])
        by_source.setdefault(source, []).append(option)
    items = list(by_source.items())
    value = nodes[items[0][0]]
    for source, options in items[1:]:
        mask = is_turn[options[0]]
        for option in options[1:]:
            mask = mask | is_turn[option]
        value = jnp.where(mask, nodes[source], value)
    return value


def lane_halves(ref, row):
    halves = [jnp.broadcast_to(ref[row : row + 1, h * 128 : h * 128 + 128], (4, 128)) for h in (0, 1)]
    return jnp.concatenate(halves, 0)


def add_parts(value):
    rows = value.shape[0] // 2
    return value[:rows] + value[rows:]


def mark_hits(code_ref, hits_ref):
    elements_here = code_ref.shape[1]
    for facet in range(4):
        codes = code_ref[facet : facet + 1, :] - 4 * elements_here
        rows = lax.broadcasted_iota(jnp.int32, (hits_ref.shape[0], elements_here), 0)
        hits_ref[:, facet * elements_here : (facet + 1) * elements_here] = jnp.where(
            rows == codes, 1.0, 0.0
        ).astype(jnp.bfloat16)


def pack_kernel(place, count, *refs):
    peers = len(place)
    source = refs[:count]
    near_ref, up_ref, down_ref, parts_ref = refs[2 * count - 1 : 2 * count + 3]
    hits_ref, orient_ref, turned_ref, box_ref, sems, box_sem = refs[2 * count + 3 :]
    target = (refs[count], orient_ref) + refs[count + 1 : 2 * count - 1]
    copies = [pltpu.make_async_copy(source[i], target[i], sems.at[i]) for i in range(count)]
    for copy in copies:
        copy.start()
    code_ref, fields_ref = target[0], target[2]
    elements_here = code_ref.shape[1]
    width = elements_here // 8
    blocks = peers + 2
    copies[0].wait()
    mark_hits(code_ref, hits_ref)
    copies[1].wait()
    copies[2].wait()
    for facet in range(4):
        own_turn = lane_halves(orient_ref, facet)
        is_turn = [own_turn == option for option in range(6)]
        nodes = []
        for j in range(FACE_NODES):
            node = int(FACE_INDEX[facet, j])
            nodes.append(fields_ref[node * 8 : node * 8 + 8, :])
        for j in range(ROWS):
            if j < FACE_NODES:
                value = select_turn(nodes, is_turn, j)
            else:
                value = jnp.zeros((8, 128), jnp.float32)
            turned_ref[facet, pl.ds(j, 8, stride=PITCH), :] = value
    turned = jnp.concatenate(
        [
            jnp.concatenate(
                [turned_ref[f, (h * 4 + c) * PITCH : (h * 4 + c) * PITCH + ROWS, :] for c in range(4)], 0
            )
            for f in range(4)
            for h in range(2)
        ],
        1,
    )
    parts = jnp.concatenate(split_two(turned), 0)
    parts_ref[...] = parts
    packed = add_parts(
        lax.dot_general(
            parts, hits_ref[...], (((1,), (1,)), ((), ())), preferred_element_type=jnp.float32
        )
    )
    for block in range(blocks):
        columns = slice(block * width, (block + 1) * width)
        value = jnp.concatenate(
            [packed[c * ROWS : (c + 1) * ROWS, columns] for c in range(4)], 1
        )
        if block < peers:
            box_ref[place[block]] = value
        elif block == peers:
            down_ref[...] = value
        else:
            up_ref[...] = value
    out = pltpu.make_async_copy(box_ref, near_ref, box_sem)
    out.start()
    for copy in copies[3:]:
        copy.wait()
    out.wait()


def inner_kernel(
    code_ref,
    fields_ref,
    store_ref,
    metric_ref,
    normal_ref,
    scale_ref,
    damping_ref,
    mask_ref,
    level_ref,
    derivative_ref,
    lift_ref,
    parts_ref,
    base_ref,
    plain_ref,
    flux_ref,
    weight_ref,
    absorb_ref,
    lift_out_ref,
    trace_ref,
):
    elements_here = code_ref.shape[1]
    total_faces = 4 * elements_here
    growth = jnp.exp2(level_ref[...].astype(jnp.float32))
    absorb = damping_ref[...] * mask_ref[...].astype(jnp.float32)
    absorb_ref[...] = absorb
    weight = 0.5 * (scale_ref[...] * growth)
    weight_ref[...] = weight

    def by_field(ref, c):
        return jnp.concatenate(
            [ref[pl.ds(h * 4 + c, VOLUME_NODES, stride=8), :] for h in range(2)], 1
        )

    for facet in range(4):
        for j in range(ROWS):
            if j < FACE_NODES:
                node = int(FACE_INDEX[facet, j])
                value = fields_ref[node * 8 : node * 8 + 8, :]
            else:
                value = jnp.zeros((8, 128), jnp.float32)
            trace_ref[pl.ds(facet * ROWS + j, 8, stride=TRACE_PITCH), :] = value
    parts = parts_ref[...]
    for facet in range(4):
        codes = code_ref[facet : facet + 1, :]
        hits = jnp.where(
            lax.broadcasted_iota(jnp.int32, (total_faces, elements_here), 0) == codes, 1.0, 0.0
        ).astype(jnp.bfloat16)
        found = add_parts(jnp.dot(parts, hits, preferred_element_type=jnp.float32))
        inside = []
        for c in range(4):
            starts = [(h * 4 + c) * TRACE_PITCH + facet * ROWS for h in range(2)]
            inside.append(jnp.concatenate([trace_ref[a : a + ROWS, :] for a in starts], 1))
        outside = [found[c * ROWS : (c + 1) * ROWS] for c in range(4)]
        normal = [normal_ref[x, facet : facet + 1, :] for x in range(3)]
        wall = codes < 0
        normal_in = normal[0] * inside[1] + normal[1] * inside[2] + normal[2] * inside[3]
        press_jump = jnp.where(wall, 0.0, inside[0] - outside[0])
        normal_jump = jnp.zeros_like(press_jump)
        for x in range(3):
            step = jnp.where(wall, 2.0 * normal[x] * normal_in, inside[1 + x] - outside[1 + x])
            normal_jump = normal_jump + normal[x] * step
        flux_ref[facet * ROWS : (facet + 1) * ROWS, :] = weight[facet : facet + 1] * (
            normal_jump - press_jump
        )
    plain = [by_field(fields_ref, c) for c in range(4)]
    for c in range(4):
        plain_ref[c] = plain[c]
    joined = jnp.concatenate(plain, 1)
    padded = jnp.concatenate([joined, jnp.zeros((5, joined.shape[1]), jnp.float32)], 0)
    high = padded.astype(jnp.bfloat16).astype(jnp.float32)
    stacked = jnp.concatenate([high, padded - high, high], 0).astype(jnp.bfloat16)
    slopes = []
    gap = jnp.zeros((VOLUME_NODES, 5), jnp.float32)
    for y in range(3):
        whole = derivative_ref[y]
        lead = whole.astype(jnp.bfloat16).astype(jnp.float32)
        left = jnp.concatenate([lead, gap, lead, gap, whole - lead, gap], 1).astype(jnp.bfloat16)
        slopes.append(jnp.dot(left, stacked, preferred_element_type=jnp.float32))

    def slope(y, c):
        return slopes[y][:, c * elements_here : (c + 1) * elements_here]

    metric = metric_ref[...] * growth

    def physical(x, c):
        total = metric[3 * x : 3 * x + 1] * slope(0, c)
        for y in (1, 2):
            total = total + metric[3 * x + y : 3 * x + y + 1] * slope(y, c)
        return total

    for c in range(4):
        if c == 0:
            volume = physical(0, 1) + physical(1, 2) + physical(2, 3)
        else:
            volume = physical(c - 1, 0)
        change = -volume - absorb * plain[c]
        base_ref[c] = RUNGE_CARRY * by_field(store_ref, c) + TIME_STEP * change
    none = jnp.zeros((VOLUME_NODES, 1), jnp.float32)
    pieces = []
    for facet in range(4):
        pieces += [lift_ref[:, facet * FACE_NODES : (facet + 1) * FACE_NODES], none]
    high, middle = split_two(jnp.concatenate(pieces, 1))
    lift_out_ref[...] = jnp.concatenate([high, high, middle, middle], 1)


def outer_kernel(
    place,
    hold_hits,
    near_ref,
    below_ref,
    above_ref,
    hits_ref,
    normal_ref,
    weight_ref,
    flux_ref,
    lift_ref,
    base_ref,
    plain_ref,
    absorb_ref,
    fields_ref,
    store_ref,
    energy_ref,
    *scratch,
):
    elements_here = plain_ref.shape[2]
    width = elements_here // 8
    if not hold_hits:
        mark_hits(hits_ref, scratch[0])
        hits_ref = scratch[0]
    boxes = [near_ref[p] for p in place] + [below_ref[...], above_ref[...]]
    received = jnp.concatenate(
        [
            jnp.concatenate([box[:, c * width : (c + 1) * width] for box in boxes], 1)
            for c in range(4)
        ],
        0,
    )
    parts = jnp.concatenate(split_two(received), 0)
    found = add_parts(jnp.dot(parts, hits_ref[...], preferred_element_type=jnp.float32))
    pieces = []
    for facet in range(4):
        columns = slice(facet * elements_here, (facet + 1) * elements_here)
        outside = [found[c * ROWS : (c + 1) * ROWS, columns] for c in range(4)]
        normal = [normal_ref[x, facet : facet + 1, :] for x in range(3)]
        across = normal[0] * outside[1] + normal[1] * outside[2] + normal[2] * outside[3]
        weight = weight_ref[facet : facet + 1, :]
        press = flux_ref[facet * ROWS : (facet + 1) * ROWS, :] + weight * (outside[0] - across)
        pieces.append([press] + [-normal[x] * press for x in range(3)])
    flux = jnp.concatenate(
        [jnp.concatenate([pieces[facet][c] for facet in range(4)], 0) for c in range(4)], 1
    )
    high, middle = split_two(flux)
    lifted = jnp.dot(
        lift_ref[...],
        jnp.concatenate([high, middle, high, middle], 0),
        preferred_element_type=jnp.float32,
    )
    square = jnp.zeros((VOLUME_NODES, elements_here), jnp.float32)
    for c in range(4):
        columns = slice(c * elements_here, (c + 1) * elements_here)
        store_next = base_ref[c] + TIME_STEP * lifted[:, columns]
        fields_next = plain_ref[c] + RUNGE_ADVANCE * store_next
        for h in range(2):
            lanes = slice(h * 128, h * 128 + 128)
            store_ref[pl.ds(h * 4 + c, VOLUME_NODES, stride=8), :] = store_next[:, lanes]
            fields_ref[pl.ds(h * 4 + c, VOLUME_NODES, stride=8), :] = fields_next[:, lanes]
        square = square + fields_next * fields_next
    energy = jnp.sum(square, 0, keepdims=True) * absorb_ref[...]
    total = energy[:, :128] + energy[:, 128:]
    energy_ref[...] = jnp.broadcast_to(total[None], energy_ref.shape)


def finish_kernel(
    divisor, shares_ref, fields_in, store_in, total_out, fields_out, store_out, total_ref, sems
):
    one = pltpu.make_async_copy(fields_in, fields_out, sems.at[0])
    two = pltpu.make_async_copy(store_in, store_out, sems.at[1])
    three = pltpu.make_async_copy(total_ref, total_out, sems.at[2])
    one.start()
    two.start()
    total_ref[0] = jnp.sum(shares_ref[...]) * (1.0 / divisor)
    three.start()
    one.wait()
    two.wait()
    three.wait()


def group_order(peers):
    lead = max(peers // 2 - 1, 0)
    rest = [member for member in range(peers) if member != lead]
    order = [lead]
    while rest:
        order.append(rest.pop())
        if rest:
            order.append(rest.pop(0))
    return order, [order.index(member) for member in range(peers)]


def as_rows(value):
    fields, nodes, elements = value.shape
    value = jnp.transpose(value.reshape(fields, nodes, elements // 128, 128), (1, 2, 0, 3))
    return value.reshape(nodes * 8, 128)


def from_rows(value, nodes):
    value = jnp.transpose(value.reshape(nodes, 2, 4, 128), (2, 0, 1, 3))
    return value.reshape(4, nodes, 256)


def in_vmem(*values):
    return [pltpu.with_memory_space_constraint(value, pltpu.VMEM) for value in values]


def local(
    fields,
    section_store,
    metric_terms,
    normals,
    face_scale,
    damping,
    absorb_mask,
    refine_level,
    face_source,
    orientation,
    derivative,
    lift_matrix,
):
    elements_here = fields.shape[2]
    assert elements_here == 256
    total_faces = 4 * elements_here
    peers = lax.axis_size("sub")
    slabs = lax.axis_size("grp")
    order, place = group_order(peers)
    devices = peers * slabs
    slots = (peers + 2) * (elements_here // 8)
    f32 = jnp.float32
    bf16 = jnp.bfloat16
    hits_shape = pltpu.VMEM((slots, total_faces), bf16)
    hold_hits = 2 * slots * total_faces <= 2**20
    row = (1, elements_here)
    given = [
        face_source,
        orientation,
        as_rows(fields),
        as_rows(section_store),
        metric_terms,
        jnp.transpose(normals, (1, 0, 2)),
        face_scale,
        damping.reshape(row),
        absorb_mask.reshape(row),
        refine_level.reshape(row),
        derivative,
        lift_matrix,
    ]
    count = len(given)
    kept = given[:1] + given[2:]
    packed = pl.pallas_call(
        lambda *refs: pack_kernel(place, count, *refs),
        out_shape=tuple(pltpu.VMEM(value.shape, value.dtype) for value in kept)
        + (
            jax.ShapeDtypeStruct((peers, ROWS, 128), f32),
            pltpu.VMEM((ROWS, 128), f32),
            pltpu.VMEM((ROWS, 128), f32),
            pltpu.VMEM((8 * ROWS, total_faces), bf16),
        )
        + ((hits_shape,) if hold_hits else ()),
        in_specs=[pl.BlockSpec(memory_space=pltpu.HBM)] * count,
        out_specs=tuple([pl.BlockSpec(memory_space=pltpu.VMEM)] * len(kept))
        + (pl.BlockSpec(memory_space=pltpu.HBM),)
        + tuple([pl.BlockSpec(memory_space=pltpu.VMEM)] * (4 if hold_hits else 3)),
        scratch_shapes=([] if hold_hits else [hits_shape])
        + [
            pltpu.VMEM((4, elements_here), jnp.int32),
            pltpu.VMEM((4, 8 * PITCH, 128), f32),
            pltpu.VMEM((peers, ROWS, 128), f32),
            pltpu.SemaphoreType.DMA((count,)),
            pltpu.SemaphoreType.DMA,
        ],
        name="pack",
    )(*given)
    held = packed[: len(kept)]
    near, up, down, parts = packed[len(kept) : len(kept) + 4]
    first = [(g, g + 1) for g in range(0, slabs - 1, 2)]
    second = [(g, (g + 1) % slabs) for g in range(1, slabs, 2)]
    second = [pair for pair in second if slabs % 2 == 0 or pair[1] > 0]
    odd = lax.axis_index("grp") % 2 == 1
    arrived = lax.all_to_all(
        near, "sub", split_axis=0, concat_axis=0, tiled=True, axis_index_groups=[order]
    )
    swap_a = lax.ppermute(jnp.where(odd, down, up), "grp", first + [(b, a) for a, b in first])
    swap_b = lax.ppermute(jnp.where(odd, up, down), "grp", second + [(b, a) for a, b in second])
    from_below = jnp.where(odd, swap_a, swap_b)
    from_above = jnp.where(odd, swap_b, swap_a)
    base, plain, flux, weight, absorb, lift_parts = pl.pallas_call(
        inner_kernel,
        out_shape=(
            pltpu.VMEM((4, VOLUME_NODES, elements_here), f32),
            pltpu.VMEM((4, VOLUME_NODES, elements_here), f32),
            pltpu.VMEM((4 * ROWS, elements_here), f32),
            pltpu.VMEM((4, elements_here), f32),
            pltpu.VMEM(row, f32),
            pltpu.VMEM((VOLUME_NODES, 16 * ROWS), bf16),
        ),
        scratch_shapes=[pltpu.VMEM((8 * TRACE_PITCH, 128), f32)],
        name="inner",
    )(*in_vmem(*held, parts))
    fields_next, store_next, energy = pl.pallas_call(
        lambda *refs: outer_kernel(place, hold_hits, *refs),
        out_shape=(
            pltpu.VMEM((VOLUME_NODES * 8, 128), f32),
            pltpu.VMEM((VOLUME_NODES * 8, 128), f32),
            pltpu.VMEM((devices, 1, 128), f32),
        ),
        scratch_shapes=[] if hold_hits else [hits_shape],
        name="outer",
    )(
        *in_vmem(
            arrived,
            from_below,
            from_above,
            packed[-1] if hold_hits else held[0],
            held[4],
            weight,
            flux,
            lift_parts,
            base,
            plain,
            absorb,
        )
    )
    shares = lax.all_to_all(energy, ("grp", "sub"), split_axis=0, concat_axis=0, tiled=True)
    divisor = elements_here * devices * VOLUME_NODES
    total, fields_next, store_next = pl.pallas_call(
        lambda *refs: finish_kernel(divisor, *refs),
        out_shape=(
            jax.ShapeDtypeStruct((1,), f32),
            jax.ShapeDtypeStruct((VOLUME_NODES * 8, 128), f32),
            jax.ShapeDtypeStruct((VOLUME_NODES * 8, 128), f32),
        ),
        in_specs=[pl.BlockSpec(memory_space=pltpu.VMEM)] * 3,
        out_specs=(
            pl.BlockSpec(memory_space=pltpu.HBM),
            pl.BlockSpec(memory_space=pltpu.HBM),
            pl.BlockSpec(memory_space=pltpu.HBM),
        ),
        scratch_shapes=[pltpu.SMEM((1,), f32), pltpu.SemaphoreType.DMA((3,))],
        name="finish",
    )(*in_vmem(shares, fields_next, store_next))
    return (
        from_rows(fields_next, VOLUME_NODES),
        from_rows(store_next, VOLUME_NODES),
        total[0],
    )


def solution(mesh):
    placed = (
        P(None, None, ("grp", "sub")),
        P(None, None, ("grp", "sub")),
        P(None, ("grp", "sub")),
        P(None, None, ("grp", "sub")),
        P(None, ("grp", "sub")),
        P(("grp", "sub")),
        P(("grp", "sub")),
        P(("grp", "sub")),
        P(None, ("grp", "sub")),
        P(None, ("grp", "sub")),
        P(),
        P(),
    )
    return jax.shard_map(
        local,
        mesh=mesh,
        in_specs=placed,
        out_specs=(P(None, None, ("grp", "sub")), P(None, None, ("grp", "sub")), P()),
        check_vma=False,
    )
```

```python
import jax
import jax.numpy as jnp
import numpy as np
from jax import lax
from jax.experimental import pallas as pl
from jax.experimental.pallas import tpu as pltpu
from jax.sharding import PartitionSpec as P


VOLUME_NODES = 35
FACE_NODES = 15
ROWS = 16
PITCH = 24
TRACE_PITCH = 72

RUNGE_CARRY = -567301805773.0 / 1357537059087.0
RUNGE_ADVANCE = 5161836677717.0 / 13612068292357.0
TIME_STEP = 0.02
INVERSE_TURN = (0, 2, 1, 3, 4, 5)


def node_tables():
    volume_list = [
        (a, b, c, 4 - a - b - c)
        for a in range(5)
        for b in range(5 - a)
        for c in range(5 - a - b)
    ]
    triples = [(a, b, 4 - a - b) for a in range(5) for b in range(5 - a)]
    face_index = np.zeros((4, 15), np.int32)
    for facet in range(4):
        others = [corner for corner in range(4) if corner != facet]
        for node_pos in range(15):
            corners = [0, 0, 0, 0]
            for place_pos in range(3):
                corners[others[place_pos]] = triples[node_pos][place_pos]
            face_index[facet, node_pos] = volume_list.index(tuple(corners))
    vertex_orders = [(0, 1, 2), (1, 2, 0), (2, 0, 1), (0, 2, 1), (2, 1, 0), (1, 0, 2)]
    turn_index = np.zeros((6, 15), np.int32)
    for option in range(6):
        order = vertex_orders[option]
        for node_pos in range(15):
            triple = triples[node_pos]
            turned = (triple[order[0]], triple[order[1]], triple[order[2]])
            turn_index[option, node_pos] = triples.index(turned)
    return face_index, turn_index


FACE_INDEX, TURN_INDEX = node_tables()


def split_two(value):
    high = value.astype(jnp.bfloat16)
    return high, (value - high.astype(jnp.float32)).astype(jnp.bfloat16)


def select_turn(nodes, is_turn, j):
    by_source = {}
    for option in range(6):
        source = int(TURN_INDEX[INVERSE_TURN[option], j])
        by_source.setdefault(source, []).append(option)
    items = list(by_source.items())
    value = nodes[items[0][0]]
    for source, options in items[1:]:
        mask = is_turn[options[0]]
        for option in options[1:]:
            mask = mask | is_turn[option]
        value = jnp.where(mask, nodes[source], value)
    return value


def lane_halves(ref, row):
    halves = [jnp.broadcast_to(ref[row : row + 1, h * 128 : h * 128 + 128], (4, 128)) for h in (0, 1)]
    return jnp.concatenate(halves, 0)


def add_parts(value):
    rows = value.shape[0] // 2
    return value[:rows] + value[rows:]


def mark_hits(code_ref, hits_ref):
    elements_here = code_ref.shape[1]
    slots = hits_ref.shape[0]
    peers = slots // (2 * ROWS) - 2
    for facet in range(4):
        slot = code_ref[facet : facet + 1, :] - 4 * elements_here
        block = slot >> 5
        half = (slot >> 4) & 1
        rank = slot & (ROWS - 1)
        inside = half * (peers * ROWS) + block * ROWS + rank
        across = 2 * peers * ROWS + half * (2 * ROWS) + (block - peers) * ROWS + rank
        row = jnp.where(slot < 0, -1, jnp.where(block < peers, inside, across))
        rows = lax.broadcasted_iota(jnp.int32, (slots, elements_here), 0)
        hits_ref[:, facet * elements_here : (facet + 1) * elements_here] = jnp.where(
            rows == row, 1.0, 0.0
        ).astype(jnp.bfloat16)


def pack_kernel(place, count, *refs):
    peers = len(place)
    source = refs[:count]
    near_ref, up_ref, down_ref, parts_ref = refs[2 * count - 1 : 2 * count + 3]
    hits_ref, orient_ref, turned_ref, box_ref, sems, box_sem = refs[2 * count + 3 :]
    target = (refs[count], orient_ref) + refs[count + 1 : 2 * count - 1]
    copies = [pltpu.make_async_copy(source[i], target[i], sems.at[i]) for i in range(count)]
    for i, copy in enumerate(copies):
        copy.start(priority=0 if i < 3 else 1)
    code_ref, fields_ref = target[0], target[2]
    elements_here = code_ref.shape[1]
    copies[0].wait()
    mark_hits(code_ref, hits_ref)
    copies[1].wait()
    copies[2].wait()
    for facet in range(4):
        own_turn = lane_halves(orient_ref, facet)
        is_turn = [own_turn == option for option in range(6)]
        nodes = []
        for j in range(FACE_NODES):
            node = int(FACE_INDEX[facet, j])
            nodes.append(fields_ref[node * 8 : node * 8 + 8, :])
        for j in range(ROWS):
            if j < FACE_NODES:
                value = select_turn(nodes, is_turn, j)
            else:
                value = jnp.zeros((8, 128), jnp.float32)
            turned_ref[facet, pl.ds(j, 8, stride=PITCH), :] = value
    turned = jnp.concatenate(
        [
            jnp.concatenate(
                [turned_ref[f, (h * 4 + c) * PITCH : (h * 4 + c) * PITCH + ROWS, :] for c in range(4)], 0
            )
            for f in range(4)
            for h in range(2)
        ],
        1,
    )
    parts = jnp.concatenate(split_two(turned), 0)
    parts_ref[...] = parts
    spread = None
    for facet in range(4):
        columns = slice(facet * elements_here, (facet + 1) * elements_here)
        piece = lax.dot_general(
            hits_ref[:, columns],
            parts[:, columns],
            (((1,), (1,)), ((), ())),
            preferred_element_type=jnp.float32,
        )
        spread = piece if spread is None else spread + piece
    spread = spread + pltpu.roll(spread, 4 * ROWS, 1)
    count_near = peers * ROWS

    def boxes(first, rows):
        lanes = lax.broadcasted_iota(jnp.int32, (rows, 128), 1)
        upper = spread[first : first + rows]
        return jnp.where(lanes < 4 * ROWS, upper, spread[first + rows : first + 2 * rows])

    near = boxes(0, count_near)
    for block in range(peers):
        box_ref[place[block]] = near[block * ROWS : (block + 1) * ROWS]
    slabs = boxes(2 * count_near, 2 * ROWS)
    down_ref[...] = slabs[:ROWS]
    up_ref[...] = slabs[ROWS:]
    out = pltpu.make_async_copy(box_ref, near_ref, box_sem)
    out.start()
    for copy in copies[3:]:
        copy.wait()
    out.wait()


def inner_kernel(
    code_ref,
    fields_ref,
    store_ref,
    metric_ref,
    normal_ref,
    scale_ref,
    damping_ref,
    mask_ref,
    level_ref,
    derivative_ref,
    lift_ref,
    parts_ref,
    base_ref,
    plain_ref,
    flux_ref,
    weight_ref,
    absorb_ref,
    lift_out_ref,
    trace_ref,
):
    elements_here = code_ref.shape[1]
    total_faces = 4 * elements_here
    growth = jnp.exp2(level_ref[...].astype(jnp.float32))
    absorb = damping_ref[...] * mask_ref[...].astype(jnp.float32)
    absorb_ref[...] = absorb
    weight = 0.5 * (scale_ref[...] * growth)
    weight_ref[...] = weight

    def by_field(ref, c):
        return jnp.concatenate(
            [ref[pl.ds(h * 4 + c, VOLUME_NODES, stride=8), :] for h in range(2)], 1
        )

    for facet in range(4):
        for j in range(ROWS):
            if j < FACE_NODES:
                node = int(FACE_INDEX[facet, j])
                value = fields_ref[node * 8 : node * 8 + 8, :]
            else:
                value = jnp.zeros((8, 128), jnp.float32)
            trace_ref[pl.ds(facet * ROWS + j, 8, stride=TRACE_PITCH), :] = value
    parts = parts_ref[...]
    for facet in range(4):
        codes = code_ref[facet : facet + 1, :]
        hits = jnp.where(
            lax.broadcasted_iota(jnp.int32, (total_faces, elements_here), 0) == codes, 1.0, 0.0
        ).astype(jnp.bfloat16)
        found = add_parts(jnp.dot(parts, hits, preferred_element_type=jnp.float32))
        inside = []
        for c in range(4):
            starts = [(h * 4 + c) * TRACE_PITCH + facet * ROWS for h in range(2)]
            inside.append(jnp.concatenate([trace_ref[a : a + ROWS, :] for a in starts], 1))
        outside = [found[c * ROWS : (c + 1) * ROWS] for c in range(4)]
        normal = [normal_ref[x, facet : facet + 1, :] for x in range(3)]
        wall = codes < 0
        normal_in = normal[0] * inside[1] + normal[1] * inside[2] + normal[2] * inside[3]
        press_jump = jnp.where(wall, 0.0, inside[0] - outside[0])
        normal_jump = jnp.zeros_like(press_jump)
        for x in range(3):
            step = jnp.where(wall, 2.0 * normal[x] * normal_in, inside[1 + x] - outside[1 + x])
            normal_jump = normal_jump + normal[x] * step
        flux_ref[facet * ROWS : (facet + 1) * ROWS, :] = weight[facet : facet + 1] * (
            normal_jump - press_jump
        )
    plain = [by_field(fields_ref, c) for c in range(4)]
    for c in range(4):
        plain_ref[c] = plain[c]
    joined = jnp.concatenate(plain, 1)
    padded = jnp.concatenate([joined, jnp.zeros((5, joined.shape[1]), jnp.float32)], 0)
    high = padded.astype(jnp.bfloat16).astype(jnp.float32)
    stacked = jnp.concatenate([high, padded - high, high], 0).astype(jnp.bfloat16)
    slopes = []
    gap = jnp.zeros((VOLUME_NODES, 5), jnp.float32)
    for y in range(3):
        whole = derivative_ref[y]
        lead = whole.astype(jnp.bfloat16).astype(jnp.float32)
        left = jnp.concatenate([lead, gap, lead, gap, whole - lead, gap], 1).astype(jnp.bfloat16)
        slopes.append(jnp.dot(left, stacked, preferred_element_type=jnp.float32))

    def slope(y, c):
        return slopes[y][:, c * elements_here : (c + 1) * elements_here]

    metric = metric_ref[...] * growth

    def physical(x, c):
        total = metric[3 * x : 3 * x + 1] * slope(0, c)
        for y in (1, 2):
            total = total + metric[3 * x + y : 3 * x + y + 1] * slope(y, c)
        return total

    for c in range(4):
        if c == 0:
            volume = physical(0, 1) + physical(1, 2) + physical(2, 3)
        else:
            volume = physical(c - 1, 0)
        change = -volume - absorb * plain[c]
        base_ref[c] = RUNGE_CARRY * by_field(store_ref, c) + TIME_STEP * change
    none = jnp.zeros((VOLUME_NODES, 1), jnp.float32)
    pieces = []
    for facet in range(4):
        pieces += [lift_ref[:, facet * FACE_NODES : (facet + 1) * FACE_NODES], none]
    high, middle = split_two(jnp.concatenate(pieces, 1))
    lift_out_ref[...] = jnp.concatenate([high, high, middle, middle], 1)


def outer_kernel(
    place,
    hold_hits,
    near_ref,
    below_ref,
    above_ref,
    hits_ref,
    normal_ref,
    weight_ref,
    flux_ref,
    lift_ref,
    base_ref,
    plain_ref,
    absorb_ref,
    fields_ref,
    store_ref,
    energy_ref,
    *scratch,
):
    elements_here = plain_ref.shape[2]
    if not hold_hits:
        mark_hits(hits_ref, scratch[0])
        hits_ref = scratch[0]
    near = jnp.concatenate([near_ref[p] for p in place], 0).T
    slabs = jnp.concatenate([below_ref[...], above_ref[...]], 0).T
    half = 4 * ROWS
    received = jnp.concatenate([near[:half], near[half:], slabs[:half], slabs[half:]], 1)
    parts = jnp.concatenate(split_two(received), 0)
    found = add_parts(jnp.dot(parts, hits_ref[...], preferred_element_type=jnp.float32))
    pieces = []
    for facet in range(4):
        columns = slice(facet * elements_here, (facet + 1) * elements_here)
        outside = [found[c * ROWS : (c + 1) * ROWS, columns] for c in range(4)]
        normal = [normal_ref[x, facet : facet + 1, :] for x in range(3)]
        across = normal[0] * outside[1] + normal[1] * outside[2] + normal[2] * outside[3]
        weight = weight_ref[facet : facet + 1, :]
        press = flux_ref[facet * ROWS : (facet + 1) * ROWS, :] + weight * (outside[0] - across)
        pieces.append([press] + [-normal[x] * press for x in range(3)])
    flux = jnp.concatenate(
        [jnp.concatenate([pieces[facet][c] for facet in range(4)], 0) for c in range(4)], 1
    )
    high, middle = split_two(flux)
    lifted = jnp.dot(
        lift_ref[...],
        jnp.concatenate([high, middle, high, middle], 0),
        preferred_element_type=jnp.float32,
    )
    square = jnp.zeros((VOLUME_NODES, elements_here), jnp.float32)
    for c in range(4):
        columns = slice(c * elements_here, (c + 1) * elements_here)
        store_next = base_ref[c] + TIME_STEP * lifted[:, columns]
        fields_next = plain_ref[c] + RUNGE_ADVANCE * store_next
        for h in range(2):
            lanes = slice(h * 128, h * 128 + 128)
            store_ref[pl.ds(h * 4 + c, VOLUME_NODES, stride=8), :] = store_next[:, lanes]
            fields_ref[pl.ds(h * 4 + c, VOLUME_NODES, stride=8), :] = fields_next[:, lanes]
        square = square + fields_next * fields_next
    energy = jnp.sum(square, 0, keepdims=True) * absorb_ref[...]
    total = energy[:, :128] + energy[:, 128:]
    energy_ref[...] = jnp.broadcast_to(total[None], energy_ref.shape)


def finish_kernel(
    divisor, shares_ref, fields_in, store_in, total_out, fields_out, store_out, total_ref, sems
):
    one = pltpu.make_async_copy(fields_in, fields_out, sems.at[0])
    two = pltpu.make_async_copy(store_in, store_out, sems.at[1])
    three = pltpu.make_async_copy(total_ref, total_out, sems.at[2])
    one.start()
    two.start()
    total_ref[0] = jnp.sum(shares_ref[...]) * (1.0 / divisor)
    three.start()
    one.wait()
    two.wait()
    three.wait()


def group_order(peers):
    lead = max(peers // 2 - 1, 0)
    rest = [member for member in range(peers) if member != lead]
    order = [lead]
    while rest:
        order.append(rest.pop())
        if rest:
            order.append(rest.pop(0))
    return order, [order.index(member) for member in range(peers)]


def as_rows(value):
    fields, nodes, elements = value.shape
    value = jnp.transpose(value.reshape(fields, nodes, elements // 128, 128), (1, 2, 0, 3))
    return value.reshape(nodes * 8, 128)


def from_rows(value, nodes):
    value = jnp.transpose(value.reshape(nodes, 2, 4, 128), (2, 0, 1, 3))
    return value.reshape(4, nodes, 256)


def in_vmem(*values):
    return [pltpu.with_memory_space_constraint(value, pltpu.VMEM) for value in values]


def local(
    fields,
    section_store,
    metric_terms,
    normals,
    face_scale,
    damping,
    absorb_mask,
    refine_level,
    face_source,
    orientation,
    derivative,
    lift_matrix,
):
    elements_here = fields.shape[2]
    assert elements_here == 256
    total_faces = 4 * elements_here
    peers = lax.axis_size("sub")
    slabs = lax.axis_size("grp")
    order, place = group_order(peers)
    devices = peers * slabs
    slots = (peers + 2) * (elements_here // 8)
    f32 = jnp.float32
    bf16 = jnp.bfloat16
    hits_shape = pltpu.VMEM((slots, total_faces), bf16)
    hold_hits = 2 * slots * total_faces <= 2**20
    row = (1, elements_here)
    given = [
        face_source,
        orientation,
        as_rows(fields),
        as_rows(section_store),
        metric_terms,
        jnp.transpose(normals, (1, 0, 2)),
        face_scale,
        damping.reshape(row),
        absorb_mask.reshape(row),
        refine_level.reshape(row),
        derivative,
        lift_matrix,
    ]
    count = len(given)
    kept = given[:1] + given[2:]
    packed = pl.pallas_call(
        lambda *refs: pack_kernel(place, count, *refs),
        out_shape=tuple(pltpu.VMEM(value.shape, value.dtype) for value in kept)
        + (
            jax.ShapeDtypeStruct((peers, ROWS, 128), f32),
            pltpu.VMEM((ROWS, 128), f32),
            pltpu.VMEM((ROWS, 128), f32),
            pltpu.VMEM((8 * ROWS, total_faces), bf16),
        )
        + ((hits_shape,) if hold_hits else ()),
        in_specs=[pl.BlockSpec(memory_space=pltpu.HBM)] * count,
        out_specs=tuple([pl.BlockSpec(memory_space=pltpu.VMEM)] * len(kept))
        + (pl.BlockSpec(memory_space=pltpu.HBM),)
        + tuple([pl.BlockSpec(memory_space=pltpu.VMEM)] * (4 if hold_hits else 3)),
        scratch_shapes=([] if hold_hits else [hits_shape])
        + [
            pltpu.VMEM((4, elements_here), jnp.int32),
            pltpu.VMEM((4, 8 * PITCH, 128), f32),
            pltpu.VMEM((peers, ROWS, 128), f32),
            pltpu.SemaphoreType.DMA((count,)),
            pltpu.SemaphoreType.DMA,
        ],
        name="pack",
    )(*given)
    held = packed[: len(kept)]
    near, up, down, parts = packed[len(kept) : len(kept) + 4]
    first = [(g, g + 1) for g in range(0, slabs - 1, 2)]
    second = [(g, (g + 1) % slabs) for g in range(1, slabs, 2)]
    second = [pair for pair in second if slabs % 2 == 0 or pair[1] > 0]
    odd = lax.axis_index("grp") % 2 == 1
    arrived = lax.all_to_all(
        near, "sub", split_axis=0, concat_axis=0, tiled=True, axis_index_groups=[order]
    )
    swap_a = lax.ppermute(jnp.where(odd, down, up), "grp", first + [(b, a) for a, b in first])
    swap_b = lax.ppermute(jnp.where(odd, up, down), "grp", second + [(b, a) for a, b in second])
    from_below = jnp.where(odd, swap_a, swap_b)
    from_above = jnp.where(odd, swap_b, swap_a)
    base, plain, flux, weight, absorb, lift_parts = pl.pallas_call(
        inner_kernel,
        out_shape=(
            pltpu.VMEM((4, VOLUME_NODES, elements_here), f32),
            pltpu.VMEM((4, VOLUME_NODES, elements_here), f32),
            pltpu.VMEM((4 * ROWS, elements_here), f32),
            pltpu.VMEM((4, elements_here), f32),
            pltpu.VMEM(row, f32),
            pltpu.VMEM((VOLUME_NODES, 16 * ROWS), bf16),
        ),
        scratch_shapes=[pltpu.VMEM((8 * TRACE_PITCH, 128), f32)],
        name="inner",
    )(*in_vmem(*held, parts))
    fields_next, store_next, energy = pl.pallas_call(
        lambda *refs: outer_kernel(place, hold_hits, *refs),
        out_shape=(
            pltpu.VMEM((VOLUME_NODES * 8, 128), f32),
            pltpu.VMEM((VOLUME_NODES * 8, 128), f32),
            pltpu.VMEM((devices, 1, 128), f32),
        ),
        scratch_shapes=[] if hold_hits else [hits_shape],
        name="outer",
    )(
        *in_vmem(
            arrived,
            from_below,
            from_above,
            packed[-1] if hold_hits else held[0],
            held[4],
            weight,
            flux,
            lift_parts,
            base,
            plain,
            absorb,
        )
    )
    shares = lax.all_to_all(energy, ("grp", "sub"), split_axis=0, concat_axis=0, tiled=True)
    divisor = elements_here * devices * VOLUME_NODES
    total, fields_next, store_next = pl.pallas_call(
        lambda *refs: finish_kernel(divisor, *refs),
        out_shape=(
            jax.ShapeDtypeStruct((1,), f32),
            jax.ShapeDtypeStruct((VOLUME_NODES * 8, 128), f32),
            jax.ShapeDtypeStruct((VOLUME_NODES * 8, 128), f32),
        ),
        in_specs=[pl.BlockSpec(memory_space=pltpu.VMEM)] * 3,
        out_specs=(
            pl.BlockSpec(memory_space=pltpu.HBM),
            pl.BlockSpec(memory_space=pltpu.HBM),
            pl.BlockSpec(memory_space=pltpu.HBM),
        ),
        scratch_shapes=[pltpu.SMEM((1,), f32), pltpu.SemaphoreType.DMA((3,))],
        name="finish",
    )(*in_vmem(shares, fields_next, store_next))
    return (
        from_rows(fields_next, VOLUME_NODES),
        from_rows(store_next, VOLUME_NODES),
        total[0],
    )


def solution(mesh):
    placed = (
        P(None, None, ("grp", "sub")),
        P(None, None, ("grp", "sub")),
        P(None, ("grp", "sub")),
        P(None, None, ("grp", "sub")),
        P(None, ("grp", "sub")),
        P(("grp", "sub")),
        P(("grp", "sub")),
        P(("grp", "sub")),
        P(None, ("grp", "sub")),
        P(None, ("grp", "sub")),
        P(),
        P(),
    )
    return jax.shard_map(
        local,
        mesh=mesh,
        in_specs=placed,
        out_specs=(P(None, None, ("grp", "sub")), P(None, None, ("grp", "sub")), P()),
        check_vma=False,
    )
```
